32 devices in a mesh: fsdp: 8 (over z, y), tp: 4 (over x, core).
Axes of the slice: x: 2, y: 2, z: 4, core: 2. Of those that a mesh axis runs over, the one named last changes fastest.
Arguments:
- base_o: bfloat16 [2, 8192, 8192], P(None, 'tp', 'fsdp'), may hold values from -0.0625 to 0.0625
- base_down: bfloat16 [2, 28672, 8192], P(None, 'tp', 'fsdp'), may hold values from -0.03125 to 0.03125
- factor_a_o: bfloat16 [2, 64, 4, 2048], P(None, None, None, 'fsdp'), may hold values from -0.0625 to 0.0625
- factor_b_o: bfloat16 [2, 8192, 64], P(None, 'fsdp'), may hold values from -1.1953125 to 1.1953125
- factor_a_down: bfloat16 [2, 64, 4, 7168], P(None, None, None, 'fsdp'), may hold values from -0.03125 to 0.03125
- factor_b_down: bfloat16 [2, 8192, 64], P(None, 'fsdp'), may hold values from -1.1953125 to 1.1953125
- magnitude_o: float32 [2, 8192], P(None, 'fsdp'), may hold values from 30 to 300
- magnitude_down: float32 [2, 8192], P(None, 'fsdp'), may hold values from 30 to 300
Outputs:
- merged_o: bfloat16 [2, 8192, 8192], P(None, 'tp', 'fsdp')
- merged_down: bfloat16 [2, 28672, 8192], P(None, 'tp', 'fsdp')
The draws below stay inside these ranges and needn't reach their ends.
All inputs are finite; a program needn't handle non-finite values.
Results may differ from the reference program's by a relative error of at most 0.001.
Values may be sent and summed in bfloat16 or wider, within the bound.
A program may use at most 192 MiB of HBM per device.

```python
import math
import jax
import jax.numpy as jnp
from jax import lax

D = 8192
FF = 28672
R = 64
LAYERS = 2
N_TP = 4


def level_of(rng, dims, cuts, smallest, top_value):
    def one(dim, shards_of):
        steps = jax.random.uniform(jax.random.fold_in(jax.random.fold_in(rng, 6), dim), (shards_of,), jnp.float32, smallest / len(cuts), top_value / len(cuts))
        return jnp.repeat(jnp.exp(steps), dims[dim] // shards_of).reshape((-1,) + (1,) * (len(dims) - dim - 1))

    level = one(*cuts[0])
    for cut in cuts[1:]:
        level = level * one(*cut)
    return level


def noise(stream_key, extent, width, reach, split=(), dtype=jnp.bfloat16):
    gain = level_of(stream_key, extent, split, -0.22, 0.18) if split else 1.0
    drawn = jax.random.normal(stream_key, extent, jnp.float32) * width * gain
    return jnp.minimum(jnp.maximum(drawn, -reach), reach).astype(dtype)


def setup_inputs(seed: int = 0) -> dict:
    seeds = jax.random.split(jax.random.key(seed), 9)
    return {
        "base_o": noise(seeds[0], (LAYERS, D, D), D ** -0.5, 0.0625, ((1, 4), (2, 8))),
        "base_down": noise(seeds[1], (LAYERS, FF, D), FF ** -0.5, 0.03125, ((1, 4), (2, 8))),
        "factor_a_o": noise(seeds[2], (LAYERS, R, N_TP, D // N_TP), D ** -0.5, 0.0625, ((3, 8),)),
        "factor_b_o": noise(seeds[3], (LAYERS, D, R), 0.2, 1.1953125, ((1, 8),)),
        "factor_a_down": noise(seeds[4], (LAYERS, R, N_TP, FF // N_TP), FF ** -0.5, 0.03125, ((3, 8),)),
        "factor_b_down": noise(seeds[5], (LAYERS, D, R), 0.2, 1.1953125, ((1, 8),)),
        "magnitude_o": jnp.clip(jnp.exp(math.log(300.0) - 2.3025851 * jax.random.uniform(seeds[6], (LAYERS, D), jnp.float32) ** level_of(seeds[6], (LAYERS, D), ((1, 8),), -0.2, 0.2)), 30.0, 300.0),
        "magnitude_down": jnp.clip(jnp.exp(math.log(300.0) - 2.3025851 * jax.random.uniform(seeds[7], (LAYERS, D), jnp.float32) ** level_of(seeds[7], (LAYERS, D), ((1, 8),), -0.2, 0.2)), 30.0, 300.0),
    }


def refresh(base, factor_a, factor_b, magnitude):
    full_a = factor_a.reshape(factor_a.shape[0], factor_a.shape[1], -1)

    def single(items):
        base_layer, a_layer, b_layer, m_layer = items
        delta = jnp.dot(a_layer.T, b_layer.T, preferred_element_type=jnp.float32)
        summed = base_layer.astype(jnp.float32) + 0.25 * delta
        square = lax.optimization_barrier(jnp.sum(summed * summed, axis=0))
        return (m_layer[None, :] * summed * lax.rsqrt(square + 1e-06)[None, :]).astype(jnp.bfloat16)
    return lax.map(single, (base, full_a, factor_b, magnitude))

def reference(base_o, base_down, factor_a_o, factor_b_o, factor_a_down, factor_b_down, magnitude_o, magnitude_down):
    merged_o = refresh(base_o, factor_a_o, factor_b_o, magnitude_o)
    merged_down = refresh(base_down, factor_a_down, factor_b_down, magnitude_down)
    return (merged_o, merged_down)
```

```python
import functools

import jax
import jax.numpy as jnp
from jax import lax
from jax.experimental import pallas as pl
from jax.experimental.pallas import tpu as pltpu
from jax.sharding import PartitionSpec as P

MESH = pl.DeviceIdType.MESH
F32 = jnp.float32
BF16 = jnp.bfloat16


def pieces_of(sizes, most):
    found = []
    for p, size in enumerate(sizes):
        rows = max(t for t in range(16, most + 1, 16) if size % t == 0)
        found += [(p, k * rows, rows) for k in range(size // rows)]
    return found


def gather_kernel(
    n,
    n_tp,
    sizes,
    rank,
    base_o,
    base_d,
    a_o,
    a_d,
    b_o,
    b_d,
    mag_o,
    mag_d,
    held_o,
    held_d,
    full_a,
    weights,
    scale,
    block,
    acc,
    sums,
    peers,
    read_sem,
    send_sem,
    recv_sem,
    sum_send,
    sum_recv,
):
    layers, columns = mag_o.shape
    depth = n // 2
    me, t = lax.axis_index("fsdp"), lax.axis_index("tp")
    z, y = me // 2, me % 2
    other = z * 2 + 1 - y
    has_lo, has_hi = z > 0, z < depth - 1
    starts = (0, sizes[0])
    pieces = pieces_of(sizes, 448)
    count = len(pieces)

    def to_fsdp(f):
        return {"fsdp": f}

    barrier = pltpu.get_barrier_semaphore()

    def greet(device):
        pl.semaphore_signal(barrier, inc=1, device_id=device, device_id_type=MESH)

    greet(to_fsdp(other))
    for k in range(1, n_tp):
        greet({"tp": (t + k) % n_tp})
    pl.when(has_lo)(lambda: greet(to_fsdp(me - 2)))
    pl.when(has_hi)(lambda: greet(to_fsdp(me + 2)))

    def slot_of(e, lo, side):
        return (z - e if lo else z + e) * 2 + side

    bases = (base_o, base_d)
    helds = (held_o, held_d)

    def read(p, f):
        rows = pl.ds(pl.multiple_of(f * sizes[p], 16), sizes[p])
        return pltpu.make_async_copy(
            bases[p].at[:, rows], helds[p].at[:, rows], read_sem.at[p, f]
        )

    def read_slot(f):
        for p in range(2):
            read(p, f).start()

    read_slot(me)
    read_slot(other)

    @pl.loop(1, depth)
    def _(d):
        for side in (y, 1 - y):
            pl.when(z - d >= 0)(lambda: read_slot(slot_of(d, True, side)))
            pl.when(z + d < depth)(lambda: read_slot(slot_of(d, False, side)))

    def rows_of(c):
        p, first, rows = pieces[c]
        return pl.ds(starts[p] + first, rows)

    def fill(p):
        a = (a_o, a_d)[p]
        parts = []
        for layer in range(layers):
            rows = a[layer, :, 0, :].astype(F32)
            for u in range(1, n_tp):
                rows = jnp.where(t == u, a[layer, :, u, :].astype(F32), rows)
            parts.append(rows)
        block[pl.ds(starts[p], sizes[p]), :] = jnp.concatenate(parts, axis=0).T.astype(BF16)

    def send(source, f, c, way, target):
        return pltpu.make_async_remote_copy(
            src_ref=source.at[rows_of(c)],
            dst_ref=full_a.at[f, rows_of(c)],
            send_sem=send_sem.at[way, f],
            recv_sem=recv_sem.at[f, c],
            device_id=to_fsdp(target),
            device_id_type=MESH,
        )

    def arrived(f, c):
        send(full_a.at[f], f, c, 0, other).wait_recv()

    def own_sends(c):
        send(block, me, c, 0, other).start()
        pl.when(has_lo)(lambda: send(block, me, c, 1, me - 2).start())
        pl.when(has_hi)(lambda: send(block, me, c, 2, me + 2).start())

    def sent(f, way):
        pltpu.make_async_remote_copy(
            src_ref=block,
            dst_ref=full_a.at[f],
            send_sem=send_sem.at[way, f],
            recv_sem=recv_sem.at[f, 0],
            device_id=to_fsdp(other),
            device_id_type=MESH,
        ).wait_send()

    ends = has_lo.astype(jnp.int32) + has_hi.astype(jnp.int32)
    for p in range(2):
        fill(p)
        if p == 0:
            pl.semaphore_wait(barrier, n_tp + ends)
        for c in range(count):
            if pieces[c][0] == p:
                own_sends(c)

    full_a[me] = block[...]
    for p, b in enumerate((b_o, b_d)):
        for layer in range(layers):
            weights[p, layer] = jnp.zeros((layers * rank, columns), BF16)
            weights[p, layer, pl.ds(layer * rank, rank), :] = (
                b[layer].astype(F32) * 0.25
            ).astype(BF16)
    acc[...] = jnp.zeros_like(acc)

    wide = 256 if columns % 256 == 0 else columns

    def process(f, c):
        p, first, rows = pieces[c]
        left = full_a[f, rows_of(c), :]
        held = pl.ds(pl.multiple_of(f * sizes[p] + first, 16), rows)
        for layer in range(layers):
            for k in range(0, columns, wide):
                cut = pl.ds(k, wide)
                total = jnp.dot(
                    left, weights[p, layer, :, cut], preferred_element_type=F32
                ) + helds[p][layer, held, cut].astype(F32)
                acc[p, layer, :, cut] += jnp.sum(
                    (total * total).reshape(rows // 8, 8, wide), axis=0
                )

    def landed(f):
        for p in range(2):
            read(p, f).wait()

    def whole(f):
        landed(f)
        for c in range(count):
            process(f, c)

    def from_other(e):
        def take(f):
            landed(f)
            for c in range(count):
                arrived(f, c)
                process(f, c)

        pl.when(z - e >= 0)(lambda: take(slot_of(e, True, 1 - y)))
        pl.when((e > 0) & (z + e < depth))(lambda: take(slot_of(e, False, 1 - y)))

    whole(me)

    def relays(d):
        for c in range(count):

            @pl.when(z - d >= 0)
            def _():
                f = slot_of(d, True, y)
                arrived(f, c)
                pl.when(has_hi)(lambda: send(full_a.at[f], f, c, 2, me + 2).start())
                send(full_a.at[f], f, c, 0, other).start()

            @pl.when(z + d < depth)
            def _():
                f = slot_of(d, False, y)
                arrived(f, c)
                pl.when(has_lo)(lambda: send(full_a.at[f], f, c, 1, me - 2).start())
                send(full_a.at[f], f, c, 0, other).start()

    @pl.loop(1, depth)
    def _(d):
        relays(d)
        from_other(d - 1)
        pl.when(z - d >= 0)(lambda: whole(slot_of(d, True, y)))
        pl.when(z + d < depth)(lambda: whole(slot_of(d, False, y)))

    from_other(jnp.int32(depth - 1))

    for p in range(2):
        for layer in range(layers):
            sums[p * layers + layer, :] = jnp.sum(acc[p, layer], axis=0)

    def share(k):
        return pltpu.make_async_remote_copy(
            src_ref=sums,
            dst_ref=peers.at[k - 1],
            send_sem=sum_send.at[k - 1],
            recv_sem=sum_recv.at[k - 1],
            device_id={"tp": (t + k) % n_tp},
            device_id_type=MESH,
        )

    for k in range(1, n_tp):
        share(k).start()

    sent(me, 0)
    pl.when(has_lo)(lambda: sent(me, 1))
    pl.when(has_hi)(lambda: sent(me, 2))

    @pl.loop(1, depth)
    def _(d):
        @pl.when(z - d >= 0)
        def _():
            f = slot_of(d, True, y)
            pl.when(has_hi)(lambda: sent(f, 2))
            sent(f, 0)

        @pl.when(z + d < depth)
        def _():
            f = slot_of(d, False, y)
            pl.when(has_lo)(lambda: sent(f, 1))
            sent(f, 0)

    square = sums[...]
    for k in range(1, n_tp):
        share(k).wait()
    for k in range(1, n_tp):
        square = square + peers[k - 1]
    magnitude = jnp.concatenate([mag_o[...], mag_d[...]], axis=0)
    scale[...] = magnitude * lax.rsqrt(square + 1e-06)


def finish_kernel(
    n, sizes, held_o, held_d, full_a, weights, scale, out_o, out_d, made_o, made_d, sem
):
    layers, _, columns = held_o.shape
    slots = made_o.shape[0]
    wide = 256 if columns % 256 == 0 else columns
    trio = ((held_o, out_o, made_o), (held_d, out_d, made_d))

    def write(p, i):
        _, out, made = trio[p]
        rows = pl.ds(pl.multiple_of((i % n) * sizes[p], 16), sizes[p])
        return pltpu.make_async_copy(
            made.at[i % slots], out.at[i // n, rows], sem.at[p, i % slots]
        )

    @pl.loop(0, layers * n)
    def _(i):
        layer, f = i // n, i % n

        @pl.when(i >= slots)
        def _():
            for p in range(2):
                write(p, i - slots).wait()

        for p, (held, _, made) in enumerate(trio):
            size, start = sizes[p], sum(sizes[:p])
            factor = scale[pl.ds(p * layers + layer, 1), :]
            left = full_a[f, pl.ds(start, size), :]
            inside = pl.ds(pl.multiple_of(f * size, 16), size)
            for c in range(0, columns, wide):
                cut = pl.ds(c, wide)
                total = jnp.dot(
                    left, weights[p, layer, :, cut], preferred_element_type=F32
                ) + held[layer, inside, cut].astype(F32)
                made[i % slots, :, cut] = (total * factor[:, c : c + wide]).astype(BF16)
        for p in range(2):
            write(p, i).start()

    @pl.loop(layers * n - slots, layers * n)
    def _(i):
        for p in range(2):
            write(p, i).wait()


def solution(mesh):
    n, n_tp = mesh.shape["fsdp"], mesh.shape["tp"]
    in_vmem = pl.BlockSpec(memory_space=pltpu.VMEM)
    anywhere = pl.BlockSpec(memory_space=pl.ANY)

    def local(base_o, base_d, a_o, b_o, a_d, b_d, mag_o, mag_d):
        layers, rank, _, part_o = a_o.shape
        sizes = (part_o, a_d.shape[3])
        columns = base_o.shape[2]
        depth = layers * rank
        count = len(pieces_of(sizes, 448))
        base_o = pltpu.with_memory_space_constraint(base_o, pltpu.HBM)
        base_d = pltpu.with_memory_space_constraint(base_d, pltpu.HBM)
        shapes = (
            pltpu.VMEM(base_o.shape, BF16),
            pltpu.VMEM(base_d.shape, BF16),
            pltpu.VMEM((n, sum(sizes), depth), BF16),
            pltpu.VMEM((2, layers, depth, columns), BF16),
            pltpu.VMEM((2 * layers, columns), F32),
        )
        held_o, held_d, full_a, weights, scale = pl.pallas_call(
            functools.partial(gather_kernel, n, n_tp, sizes, rank),
            out_shape=shapes,
            in_specs=[anywhere] * 2 + [in_vmem] * 6,
            out_specs=[in_vmem] * 5,
            scratch_shapes=[
                pltpu.VMEM((sum(sizes), depth), BF16),
                pltpu.VMEM((2, layers, 8, columns), F32),
                pltpu.VMEM((2 * layers, columns), F32),
                pltpu.VMEM((n_tp - 1, 2 * layers, columns), F32),
                pltpu.SemaphoreType.DMA((2, n)),
                pltpu.SemaphoreType.DMA((3, n)),
                pltpu.SemaphoreType.DMA((n, count)),
                pltpu.SemaphoreType.DMA((n_tp - 1,)),
                pltpu.SemaphoreType.DMA((n_tp - 1,)),
            ],
            compiler_params=pltpu.CompilerParams(
                collective_id=0, has_side_effects=True, vmem_limit_bytes=20 << 20
            ),
            name="gather_squares",
        )(
            base_o, base_d, a_o, a_d, b_o.swapaxes(1, 2), b_d.swapaxes(1, 2), mag_o, mag_d
        )

        kept = [
            pltpu.with_memory_space_constraint(x, pltpu.VMEM)
            for x in (held_o, held_d, full_a, weights, scale)
        ]
        return pl.pallas_call(
            functools.partial(finish_kernel, n, sizes),
            out_shape=[jax.ShapeDtypeStruct(b.shape, BF16) for b in (base_o, base_d)],
            in_specs=[in_vmem] * 5,
            out_specs=[pl.BlockSpec(memory_space=pltpu.HBM)] * 2,
            scratch_shapes=[pltpu.VMEM((4, size, columns), BF16) for size in sizes]
            + [pltpu.SemaphoreType.DMA((2, 4))],
            compiler_params=pltpu.CompilerParams(vmem_limit_bytes=20 << 20),
            name="finish",
        )(*kept)

    return jax.shard_map(
        local,
        mesh=mesh,
        in_specs=(
            P(None, "tp", "fsdp"),
            P(None, "tp", "fsdp"),
            P(None, None, None, "fsdp"),
            P(None, "fsdp", None),
            P(None, None, None, "fsdp"),
            P(None, "fsdp", None),
            P(None, "fsdp"),
            P(None, "fsdp"),
        ),
        out_specs=(P(None, "tp", "fsdp"), P(None, "tp", "fsdp")),
        check_vma=False,
    )
```

```python
import functools

import jax
import jax.numpy as jnp
from jax import lax
from jax.experimental import pallas as pl
from jax.experimental.pallas import tpu as pltpu
from jax.sharding import PartitionSpec as P

MESH = pl.DeviceIdType.MESH
F32 = jnp.float32
BF16 = jnp.bfloat16
LAST = 96


def pieces_of(sizes):
    last = sum(sizes) // LAST * 16
    late = sum(sizes) // 32 * 16
    early = sizes[1] - late
    return [(0, 0, sizes[0]), (1, 0, early), (1, early, late - last), (1, sizes[1] - last, last)]


def gather_kernel(
    n,
    n_tp,
    sizes,
    rank,
    base_o,
    base_d,
    a_o,
    a_d,
    b_o,
    b_d,
    mag_o,
    mag_d,
    held_o,
    held_d,
    full_a,
    weights,
    scale,
    block,
    acc,
    sums,
    peers,
    kept_a_o,
    kept_a_d,
    kept_b_o,
    kept_b_d,
    kept_mag,
    load_sem,
    read_sem,
    send_sem,
    recv_sem,
    sum_send,
    sum_recv,
):
    layers, columns = mag_o.shape
    depth = n // 2
    me, t = lax.axis_index("fsdp"), lax.axis_index("tp")
    z, y = me // 2, me % 2
    other = z * 2 + 1 - y
    has_lo, has_hi = z > 0, z < depth - 1
    starts = (0, sizes[0])
    pieces = pieces_of(sizes)
    count = len(pieces)
    early, late = range(count - 2), range(count - 2, count)
    cut_row = starts[1] + pieces[count - 2][1]
    mate = (z + 1 - 2 * (z % 2)) * 2

    def to_fsdp(f):
        return {"fsdp": f}

    barrier = pltpu.get_barrier_semaphore()

    def greet(device):
        pl.semaphore_signal(barrier, inc=1, device_id=device, device_id_type=MESH)

    greet(to_fsdp(other))
    for k in range(1, n_tp):
        greet({"tp": (t + k) % n_tp})
    pl.when(has_lo)(lambda: greet(to_fsdp(me - 2)))
    pl.when(has_hi)(lambda: greet(to_fsdp(me + 2)))

    loads = [
        pltpu.make_async_copy(source, target, load_sem.at[k])
        for k, (source, target) in enumerate(
            (
                (a_o, kept_a_o),
                (a_d, kept_a_d),
                (b_o, kept_b_o),
                (b_d, kept_b_d),
                (mag_o, kept_mag.at[0]),
                (mag_d, kept_mag.at[1]),
            )
        )
    ]
    for load in loads:
        load.start()

    def slot_of(e, lo, side):
        return (z - e if lo else z + e) * 2 + side

    bases = (base_o, base_d)
    helds = (held_o, held_d)

    def read(p, f):
        rows = pl.ds(pl.multiple_of(f * sizes[p], 16), sizes[p])
        return pltpu.make_async_copy(
            bases[p].at[:, rows], helds[p].at[:, rows], read_sem.at[p, f]
        )

    def read_slot(f):
        for p in range(2):
            read(p, f).start()

    read_slot(me)
    read_slot(other)

    @pl.loop(1, depth)
    def _(d):
        for side in (y, 1 - y):
            pl.when(z - d >= 0)(lambda: read_slot(slot_of(d, True, side)))
            pl.when(z + d < depth)(lambda: read_slot(slot_of(d, False, side)))

    def rows_of(c):
        p, first, rows = pieces[c]
        return pl.ds(starts[p] + first, rows)

    def fill(p):
        a = (kept_a_o, kept_a_d)[p]
        loads[p].wait()
        parts = []
        for layer in range(layers):
            rows = a[layer, :, 0, :].astype(F32)
            for u in range(1, n_tp):
                rows = jnp.where(t == u, a[layer, :, u, :].astype(F32), rows)
            parts.append(rows)
        block[pl.ds(starts[p], sizes[p]), :] = jnp.concatenate(parts, axis=0).T.astype(BF16)

    def send(source, f, c, way, target):
        return pltpu.make_async_remote_copy(
            src_ref=source.at[rows_of(c)],
            dst_ref=full_a.at[f, rows_of(c)],
            send_sem=send_sem.at[way, f],
            recv_sem=recv_sem.at[f, c],
            device_id=to_fsdp(target),
            device_id_type=MESH,
        )

    def arrived(f, c):
        send(full_a.at[f], f, c, 0, other).wait_recv()

    def own_sends(c):
        send(block, me, c, 0, other).start()
        pl.when(has_lo)(lambda: send(block, me, c, 1, me - 2).start())
        pl.when(has_hi)(lambda: send(block, me, c, 2, me + 2).start())

    def sent(f, way, rows):
        pltpu.make_async_remote_copy(
            src_ref=block.at[rows],
            dst_ref=full_a.at[f, rows],
            send_sem=send_sem.at[way, f],
            recv_sem=recv_sem.at[f, 0],
            device_id=to_fsdp(other),
            device_id_type=MESH,
        ).wait_send()

    ends = has_lo.astype(jnp.int32) + has_hi.astype(jnp.int32)
    for p in range(2):
        fill(p)
        if p == 0:
            pl.semaphore_wait(barrier, n_tp + ends)
        for c in range(count):
            if pieces[c][0] == p:
                own_sends(c)

    full_a[me] = block[...]
    for p, b in enumerate((kept_b_o, kept_b_d)):
        loads[2 + p].wait()
        for layer in range(layers):
            weights[p, layer] = jnp.zeros((layers * rank, columns), BF16)
            weights[p, layer, pl.ds(layer * rank, rank), :] = (
                b[layer].astype(F32) * 0.25
            ).astype(BF16)
    acc[...] = jnp.zeros_like(acc)

    wide = 256 if columns % 256 == 0 else columns

    def process(f, c):
        p, first, rows = pieces[c]
        left = full_a[f, rows_of(c), :]
        held = pl.ds(pl.multiple_of(f * sizes[p] + first, 16), rows)
        for layer in range(layers):
            for k in range(0, columns, wide):
                cut = pl.ds(k, wide)
                total = jnp.dot(
                    left, weights[p, layer, :, cut], preferred_element_type=F32
                ) + helds[p][layer, held, cut].astype(F32)
                acc[p, layer, :, cut] += jnp.sum(
                    (total * total).reshape(rows // 8, 8, wide), axis=0
                )

    def landed(f):
        for p in range(2):
            read(p, f).wait()

    def own_column(f, c):
        if c == 0:
            landed(f)
        process(f, c)

    def take(f, c):
        arrived(f, c)
        process(f, c)

    def other_column(f, c):
        if c == 0:
            landed(f)
        if c in early:
            take(f, c)
        else:
            pl.when(f != mate + 1 - y)(lambda: take(f, c))

    for c in range(count):
        own_column(me, c)

    def relay(f, c, way, more, target):
        arrived(f, c)
        pl.when(more)(lambda: send(full_a.at[f], f, c, way, target).start())
        if c in early:
            send(full_a.at[f], f, c, 0, other).start()
        else:
            pl.when(f != mate + y)(lambda: send(full_a.at[f], f, c, 0, other).start())

    def cross(act):
        pl.when(z % 2 == 1)(lambda: act(1, me - 2))
        pl.when(z % 2 == 0)(lambda: act(2, me + 2))

    def start_cross(way, target):
        for c in late:
            send(full_a.at[other], other, c, way, target).start()

    @pl.loop(1, depth + 1)
    def _(d):
        pl.when(d == max(depth - 1, 1))(lambda: cross(start_cross))
        for c in range(count):
            pl.when(z - d >= 0)(lambda: relay(slot_of(d, True, y), c, 2, has_hi, me + 2))
            pl.when(z + d < depth)(lambda: relay(slot_of(d, False, y), c, 1, has_lo, me - 2))
            if c in late:
                pl.when(d == depth)(lambda: take(mate + 1 - y, c))
            pl.when(z - d + 1 >= 0)(lambda: other_column(slot_of(d - 1, True, 1 - y), c))
            pl.when((d > 1) & (z + d - 1 < depth))(
                lambda: other_column(slot_of(d - 1, False, 1 - y), c)
            )
            pl.when(z - d >= 0)(lambda: own_column(slot_of(d, True, y), c))
            pl.when(z + d < depth)(lambda: own_column(slot_of(d, False, y), c))

    for p in range(2):
        for layer in range(layers):
            sums[p * layers + layer, :] = jnp.sum(acc[p, layer], axis=0)

    def share(k):
        return pltpu.make_async_remote_copy(
            src_ref=sums,
            dst_ref=peers.at[k - 1],
            send_sem=sum_send.at[k - 1],
            recv_sem=sum_recv.at[k - 1],
            device_id={"tp": (t + k) % n_tp},
            device_id_type=MESH,
        )

    for k in range(1, n_tp):
        share(k).start()

    every = pl.ds(0, sum(sizes))
    first, rest = pl.ds(0, cut_row), pl.ds(cut_row, sum(sizes) - cut_row)
    sent(me, 0, every)
    pl.when(has_lo)(lambda: sent(me, 1, every))
    pl.when(has_hi)(lambda: sent(me, 2, every))
    sent(mate + y, 0, first)
    cross(lambda way, _: sent(other, way, rest))

    def relayed(f, way, more):
        pl.when(more)(lambda: sent(f, way, every))
        pl.when(f != mate + y)(lambda: sent(f, 0, every))

    @pl.loop(1, depth)
    def _(d):
        pl.when(z - d >= 0)(lambda: relayed(slot_of(d, True, y), 2, has_hi))
        pl.when(z + d < depth)(lambda: relayed(slot_of(d, False, y), 1, has_lo))

    square = sums[...]
    for k in range(1, n_tp):
        share(k).wait()
    for k in range(1, n_tp):
        square = square + peers[k - 1]
    loads[4].wait()
    loads[5].wait()
    magnitude = jnp.concatenate([kept_mag[0], kept_mag[1]], axis=0)
    scale[...] = magnitude * lax.rsqrt(square + 1e-06)


def finish_kernel(
    n, sizes, held_o, held_d, full_a, weights, scale, out_o, out_d, made_o, made_d, sem
):
    layers, _, columns = held_o.shape
    slots = made_o.shape[0]
    wide = 256 if columns % 256 == 0 else columns
    trio = ((held_o, out_o, made_o), (held_d, out_d, made_d))

    turns = slots // layers

    def write(p, layer, f):
        _, out, made = trio[p]
        rows = pl.ds(pl.multiple_of(f * sizes[p], 16), sizes[p])
        slot = (f % turns) * layers + layer
        return pltpu.make_async_copy(made.at[slot], out.at[layer, rows], sem.at[p, slot])

    @pl.loop(0, n)
    def _(f):
        @pl.when(f >= turns)
        def _():
            for layer in range(layers):
                for p in range(2):
                    write(p, layer, f - turns).wait()

        for layer in range(layers):
            for p, (held, _, made) in enumerate(trio):
                size, start = sizes[p], sum(sizes[:p])
                factor = scale[pl.ds(p * layers + layer, 1), :]
                left = full_a[f, pl.ds(start, size), :]
                inside = pl.ds(pl.multiple_of(f * size, 16), size)
                for c in range(0, columns, wide):
                    cut = pl.ds(c, wide)
                    total = jnp.dot(
                        left, weights[p, layer, :, cut], preferred_element_type=F32
                    ) + held[layer, inside, cut].astype(F32)
                    made[(f % turns) * layers + layer, :, cut] = (
                        total * factor[:, c : c + wide]
                    ).astype(BF16)
                write(p, layer, f).start()

    @pl.loop(n - turns, n)
    def _(f):
        for layer in range(layers):
            for p in range(2):
                write(p, layer, f).wait()


def solution(mesh):
    n, n_tp = mesh.shape["fsdp"], mesh.shape["tp"]
    in_vmem = pl.BlockSpec(memory_space=pltpu.VMEM)
    anywhere = pl.BlockSpec(memory_space=pl.ANY)

    def local(base_o, base_d, a_o, b_o, a_d, b_d, mag_o, mag_d):
        layers, rank, _, part_o = a_o.shape
        sizes = (part_o, a_d.shape[3])
        columns = base_o.shape[2]
        depth = layers * rank
        count = len(pieces_of(sizes))
        b_o, b_d = b_o.swapaxes(1, 2), b_d.swapaxes(1, 2)
        given = [
            pltpu.with_memory_space_constraint(x, pltpu.HBM)
            for x in (base_o, base_d, a_o, a_d, b_o, b_d, mag_o, mag_d)
        ]
        shapes = (
            pltpu.VMEM(base_o.shape, BF16),
            pltpu.VMEM(base_d.shape, BF16),
            pltpu.VMEM((n, sum(sizes), depth), BF16),
            pltpu.VMEM((2, layers, depth, columns), BF16),
            pltpu.VMEM((2 * layers, columns), F32),
        )
        held_o, held_d, full_a, weights, scale = pl.pallas_call(
            functools.partial(gather_kernel, n, n_tp, sizes, rank),
            out_shape=shapes,
            in_specs=[anywhere] * 8,
            out_specs=[in_vmem] * 5,
            scratch_shapes=[
                pltpu.VMEM((sum(sizes), depth), BF16),
                pltpu.VMEM((2, layers, 8, columns), F32),
                pltpu.VMEM((2 * layers, columns), F32),
                pltpu.VMEM((n_tp - 1, 2 * layers, columns), F32),
                pltpu.VMEM(a_o.shape, BF16),
                pltpu.VMEM(a_d.shape, BF16),
                pltpu.VMEM(b_o.shape, BF16),
                pltpu.VMEM(b_d.shape, BF16),
                pltpu.VMEM((2, layers, columns), F32),
                pltpu.SemaphoreType.DMA((6,)),
                pltpu.SemaphoreType.DMA((2, n)),
                pltpu.SemaphoreType.DMA((3, n)),
                pltpu.SemaphoreType.DMA((n, count)),
                pltpu.SemaphoreType.DMA((n_tp - 1,)),
                pltpu.SemaphoreType.DMA((n_tp - 1,)),
            ],
            compiler_params=pltpu.CompilerParams(
                collective_id=0, has_side_effects=True, vmem_limit_bytes=20 << 20
            ),
            name="gather_squares",
        )(*given)

        kept = [
            pltpu.with_memory_space_constraint(x, pltpu.VMEM)
            for x in (held_o, held_d, full_a, weights, scale)
        ]
        return pl.pallas_call(
            functools.partial(finish_kernel, n, sizes),
            out_shape=[jax.ShapeDtypeStruct(b.shape, BF16) for b in (base_o, base_d)],
            in_specs=[in_vmem] * 5,
            out_specs=[pl.BlockSpec(memory_space=pltpu.HBM)] * 2,
            scratch_shapes=[pltpu.VMEM((4, size, columns), BF16) for size in sizes]
            + [pltpu.SemaphoreType.DMA((2, 4))],
            compiler_params=pltpu.CompilerParams(vmem_limit_bytes=20 << 20),
            name="finish",
        )(*kept)

    return jax.shard_map(
        local,
        mesh=mesh,
        in_specs=(
            P(None, "tp", "fsdp"),
            P(None, "tp", "fsdp"),
            P(None, None, None, "fsdp"),
            P(None, "fsdp", None),
            P(None, None, None, "fsdp"),
            P(None, "fsdp", None),
            P(None, "fsdp"),
            P(None, "fsdp"),
        ),
        out_specs=(P(None, "tp", "fsdp"), P(None, "tp", "fsdp")),
        check_vma=False,
    )
```

```python
import functools

import jax
import jax.numpy as jnp
from jax import lax
from jax.experimental import pallas as pl
from jax.experimental.pallas import tpu as pltpu
from jax.sharding import PartitionSpec as P

MESH = pl.DeviceIdType.MESH
F32 = jnp.float32
BF16 = jnp.bfloat16
LAST = 96


def pieces_of(sizes):
    last = sum(sizes) // LAST * 16
    late = sum(sizes) // 32 * 16
    early = sizes[1] - late
    return [(0, 0, sizes[0]), (1, 0, early), (1, early, late - last), (1, sizes[1] - last, last)]


def gather_kernel(
    n,
    n_tp,
    sizes,
    rank,
    base_o,
    base_d,
    a_o,
    a_d,
    b_o,
    b_d,
    mag_o,
    mag_d,
    held_o,
    held_d,
    full_a,
    weights,
    scale,
    block,
    acc,
    sums,
    peers,
    kept_a_o,
    kept_a_d,
    kept_b_o,
    kept_b_d,
    kept_mag,
    load_sem,
    read_sem,
    send_sem,
    recv_sem,
    sum_send,
    sum_recv,
):
    layers, columns = mag_o.shape
    depth = n // 2
    me, t = lax.axis_index("fsdp"), lax.axis_index("tp")
    z, y = me // 2, me % 2
    other = z * 2 + 1 - y
    has_lo, has_hi = z > 0, z < depth - 1
    starts = (0, sizes[0])
    pieces = pieces_of(sizes)
    count = len(pieces)
    early, late = range(count - 2), range(count - 2, count)
    mate = (z + 1 - 2 * (z % 2)) * 2

    def to_fsdp(f):
        return {"fsdp": f}

    barrier = pltpu.get_barrier_semaphore()

    def greet(device):
        pl.semaphore_signal(barrier, inc=1, device_id=device, device_id_type=MESH)

    greet(to_fsdp(other))
    for k in range(1, n_tp):
        greet({"tp": (t + k) % n_tp})
    pl.when(has_lo)(lambda: greet(to_fsdp(me - 2)))
    pl.when(has_hi)(lambda: greet(to_fsdp(me + 2)))

    loads = [
        pltpu.make_async_copy(source, target, load_sem.at[k])
        for k, (source, target) in enumerate(
            (
                (a_o, kept_a_o),
                (a_d, kept_a_d),
                (b_o, kept_b_o),
                (b_d, kept_b_d),
                (mag_o, kept_mag.at[0]),
                (mag_d, kept_mag.at[1]),
            )
        )
    ]
    for load in loads:
        load.start()

    def slot_of(e, lo, side):
        return (z - e if lo else z + e) * 2 + side

    bases = (base_o, base_d)
    helds = (held_o, held_d)

    def read(p, f):
        rows = pl.ds(pl.multiple_of(f * sizes[p], 16), sizes[p])
        return pltpu.make_async_copy(
            bases[p].at[:, rows], helds[p].at[:, rows], read_sem.at[f]
        )

    def read_slot(f):
        for p in range(2):
            read(p, f).start()

    read_slot(me)
    read_slot(other)

    @pl.loop(1, depth)
    def _(d):
        for side in (y, 1 - y):
            pl.when(z - d >= 0)(lambda: read_slot(slot_of(d, True, side)))
            pl.when(z + d < depth)(lambda: read_slot(slot_of(d, False, side)))

    def rows_of(c):
        p, first, rows = pieces[c]
        return pl.ds(starts[p] + first, rows)

    def fill(p):
        a = (kept_a_o, kept_a_d)[p]
        loads[p].wait()
        parts = []
        for layer in range(layers):
            rows = a[layer, :, 0, :].astype(F32)
            for u in range(1, n_tp):
                rows = jnp.where(t == u, a[layer, :, u, :].astype(F32), rows)
            parts.append(rows)
        block[pl.ds(starts[p], sizes[p]), :] = jnp.concatenate(parts, axis=0).T.astype(BF16)

    def send(source, f, c, lane, target):
        return pltpu.make_async_remote_copy(
            src_ref=source.at[rows_of(c)],
            dst_ref=full_a.at[f, rows_of(c)],
            send_sem=send_sem.at[lane],
            recv_sem=recv_sem.at[f, c],
            device_id=to_fsdp(target),
            device_id_type=MESH,
        )

    def arrived(f, c):
        send(full_a.at[f], f, c, 0, other).wait_recv()

    def own_sends(c):
        send(block, me, c, 0, other).start()
        pl.when(has_lo)(lambda: send(block, me, c, 1, me - 2).start())
        pl.when(has_hi)(lambda: send(block, me, c, 1, me + 2).start())

    def sent(lane, blocks):
        whole = full_a.at[pl.ds(0, blocks)]
        pltpu.make_async_remote_copy(
            src_ref=whole,
            dst_ref=whole,
            send_sem=send_sem.at[lane],
            recv_sem=recv_sem.at[0, 0],
            device_id=to_fsdp(other),
            device_id_type=MESH,
        ).wait_send()

    ends = has_lo.astype(jnp.int32) + has_hi.astype(jnp.int32)
    for p in range(2):
        fill(p)
        if p == 0:
            pl.semaphore_wait(barrier, n_tp + ends)
        for c in range(count):
            if pieces[c][0] == p:
                own_sends(c)

    full_a[me] = block[...]
    for p, b in enumerate((kept_b_o, kept_b_d)):
        loads[2 + p].wait()
        for layer in range(layers):
            weights[p, layer] = jnp.zeros((layers * rank, columns), BF16)
            weights[p, layer, pl.ds(layer * rank, rank), :] = (
                b[layer].astype(F32) * 0.25
            ).astype(BF16)
    acc[...] = jnp.zeros_like(acc)

    wide = 256 if columns % 256 == 0 else columns

    def process(f, c):
        p, first, rows = pieces[c]
        left = full_a[f, rows_of(c), :]
        held = pl.ds(pl.multiple_of(f * sizes[p] + first, 16), rows)
        for layer in range(layers):
            for k in range(0, columns, wide):
                cut = pl.ds(k, wide)
                total = jnp.dot(
                    left, weights[p, layer, :, cut], preferred_element_type=F32
                ) + helds[p][layer, held, cut].astype(F32)
                acc[p, layer, :, cut] += jnp.sum(
                    (total * total).reshape(rows // 8, 8, wide), axis=0
                )

    def landed(f):
        rows = pl.ds(0, sum(sizes))
        pltpu.make_async_copy(base_d.at[:, rows], held_d.at[:, rows], read_sem.at[f]).wait()

    def own_column(f, c):
        if c == 0:
            landed(f)
        process(f, c)

    def take(f, c):
        arrived(f, c)
        process(f, c)

    def other_column(f, c):
        if c == 0:
            landed(f)
        if c in early:
            take(f, c)
        else:
            pl.when(f != mate + 1 - y)(lambda: take(f, c))

    for c in range(count):
        own_column(me, c)

    def relay(f, c, more, target):
        arrived(f, c)
        pl.when(more)(lambda: send(full_a.at[f], f, c, 1, target).start())
        if c in early:
            send(full_a.at[f], f, c, 0, other).start()
        else:
            pl.when(f != mate + y)(lambda: send(full_a.at[f], f, c, 0, other).start())

    def cross(act):
        pl.when(z % 2 == 1)(lambda: act(me - 2))
        pl.when(z % 2 == 0)(lambda: act(me + 2))

    def start_cross(target):
        for c in late:
            send(full_a.at[other], other, c, 0, target).start()

    def share(k, p):
        return pltpu.make_async_remote_copy(
            src_ref=sums.at[p],
            dst_ref=peers.at[k - 1, p],
            send_sem=sum_send.at[k - 1, p],
            recv_sem=sum_recv.at[k - 1, p],
            device_id={"tp": (t + k) % n_tp},
            device_id_type=MESH,
        )

    def share_sums(p):
        for layer in range(layers):
            sums[p, layer, :] = jnp.sum(acc[p, layer], axis=0)
        for k in range(1, n_tp):
            share(k, p).start()

    @pl.loop(1, depth + 1)
    def _(d):
        pl.when(d == max(depth - 1, 1))(lambda: cross(start_cross))
        def relays(c):
            pl.when(z + d < depth)(lambda: relay(slot_of(d, False, y), c, has_lo, me - 2))
            pl.when(z - d >= 0)(lambda: relay(slot_of(d, True, y), c, has_hi, me + 2))

        relays(0)
        for c in range(count):
            if c + 1 < count:
                relays(c + 1)
            if c in late:
                pl.when(d == depth)(lambda: take(mate + 1 - y, c))
            pl.when(z - d + 1 >= 0)(lambda: other_column(slot_of(d - 1, True, 1 - y), c))
            pl.when((d > 1) & (z + d - 1 < depth))(
                lambda: other_column(slot_of(d - 1, False, 1 - y), c)
            )
            pl.when(z - d >= 0)(lambda: own_column(slot_of(d, True, y), c))
            pl.when(z + d < depth)(lambda: own_column(slot_of(d, False, y), c))
            if c == 0:
                pl.when(d == depth)(lambda: share_sums(0))

    share_sums(1)
    sent(0, depth)
    pl.when(has_lo & has_hi)(lambda: sent(1, depth + 1))
    pl.when(~(has_lo & has_hi))(lambda: sent(1, 1))

    loads[4].wait()
    loads[5].wait()
    for p in range(2):
        square = sums[p]
        for k in range(1, n_tp):
            share(k, p).wait()
        for k in range(1, n_tp):
            square = square + peers[k - 1, p]
        scale[pl.ds(p * layers, layers), :] = kept_mag[p] * lax.rsqrt(square + 1e-06)


def finish_kernel(
    n, sizes, held_o, held_d, full_a, weights, scale, out_o, out_d, made_o, made_d, sem
):
    layers, _, columns = held_o.shape
    slots = made_o.shape[0]
    wide = 256 if columns % 256 == 0 else columns
    trio = ((held_o, out_o, made_o), (held_d, out_d, made_d))

    turns = slots // layers

    def write(p, layer, f):
        _, out, made = trio[p]
        rows = pl.ds(pl.multiple_of(f * sizes[p], 16), sizes[p])
        slot = (f % turns) * layers + layer
        return pltpu.make_async_copy(made.at[slot], out.at[layer, rows], sem.at[p, slot])

    @pl.loop(0, n)
    def _(f):
        @pl.when(f >= turns)
        def _():
            for layer in range(layers):
                for p in range(2):
                    write(p, layer, f - turns).wait()

        for layer in range(layers):
            for p, (held, _, made) in enumerate(trio):
                size, start = sizes[p], sum(sizes[:p])
                factor = scale[pl.ds(p * layers + layer, 1), :]
                left = full_a[f, pl.ds(start, size), :]
                inside = pl.ds(pl.multiple_of(f * size, 16), size)
                for c in range(0, columns, wide):
                    cut = pl.ds(c, wide)
                    total = jnp.dot(
                        left, weights[p, layer, :, cut], preferred_element_type=F32
                    ) + held[layer, inside, cut].astype(F32)
                    made[(f % turns) * layers + layer, :, cut] = (
                        total * factor[:, c : c + wide]
                    ).astype(BF16)
                write(p, layer, f).start()

    @pl.loop(n - turns, n)
    def _(f):
        for layer in range(layers):
            for p in range(2):
                write(p, layer, f).wait()


def solution(mesh):
    n, n_tp = mesh.shape["fsdp"], mesh.shape["tp"]
    in_vmem = pl.BlockSpec(memory_space=pltpu.VMEM)
    anywhere = pl.BlockSpec(memory_space=pl.ANY)

    def local(base_o, base_d, a_o, b_o, a_d, b_d, mag_o, mag_d):
        layers, rank, _, part_o = a_o.shape
        sizes = (part_o, a_d.shape[3])
        columns = base_o.shape[2]
        depth = layers * rank
        count = len(pieces_of(sizes))
        b_o, b_d = b_o.swapaxes(1, 2), b_d.swapaxes(1, 2)
        given = [
            pltpu.with_memory_space_constraint(x, pltpu.HBM)
            for x in (base_o, base_d, a_o, a_d, b_o, b_d, mag_o, mag_d)
        ]
        shapes = (
            pltpu.VMEM(base_o.shape, BF16),
            pltpu.VMEM(base_d.shape, BF16),
            pltpu.VMEM((n, sum(sizes), depth), BF16),
            pltpu.VMEM((2, layers, depth, columns), BF16),
            pltpu.VMEM((2 * layers, columns), F32),
        )
        held_o, held_d, full_a, weights, scale = pl.pallas_call(
            functools.partial(gather_kernel, n, n_tp, sizes, rank),
            out_shape=shapes,
            in_specs=[anywhere] * 8,
            out_specs=[in_vmem] * 5,
            scratch_shapes=[
                pltpu.VMEM((sum(sizes), depth), BF16),
                pltpu.VMEM((2, layers, 8, columns), F32),
                pltpu.VMEM((2, layers, columns), F32),
                pltpu.VMEM((n_tp - 1, 2, layers, columns), F32),
                pltpu.VMEM(a_o.shape, BF16),
                pltpu.VMEM(a_d.shape, BF16),
                pltpu.VMEM(b_o.shape, BF16),
                pltpu.VMEM(b_d.shape, BF16),
                pltpu.VMEM((2, layers, columns), F32),
                pltpu.SemaphoreType.DMA((6,)),
                pltpu.SemaphoreType.DMA((n,)),
                pltpu.SemaphoreType.DMA((2,)),
                pltpu.SemaphoreType.DMA((n, count)),
                pltpu.SemaphoreType.DMA((n_tp - 1, 2)),
                pltpu.SemaphoreType.DMA((n_tp - 1, 2)),
            ],
            compiler_params=pltpu.CompilerParams(
                collective_id=0, has_side_effects=True, vmem_limit_bytes=20 << 20
            ),
            name="gather_squares",
        )(*given)

        kept = [
            pltpu.with_memory_space_constraint(x, pltpu.VMEM)
            for x in (held_o, held_d, full_a, weights, scale)
        ]
        return pl.pallas_call(
            functools.partial(finish_kernel, n, sizes),
            out_shape=[jax.ShapeDtypeStruct(b.shape, BF16) for b in (base_o, base_d)],
            in_specs=[in_vmem] * 5,
            out_specs=[pl.BlockSpec(memory_space=pltpu.HBM)] * 2,
            scratch_shapes=[pltpu.VMEM((4, size, columns), BF16) for size in sizes]
            + [pltpu.SemaphoreType.DMA((2, 4))],
            compiler_params=pltpu.CompilerParams(vmem_limit_bytes=20 << 20),
            name="finish",
        )(*kept)

    return jax.shard_map(
        local,
        mesh=mesh,
        in_specs=(
            P(None, "tp", "fsdp"),
            P(None, "tp", "fsdp"),
            P(None, None, None, "fsdp"),
            P(None, "fsdp", None),
            P(None, None, None, "fsdp"),
            P(None, "fsdp", None),
            P(None, "fsdp"),
            P(None, "fsdp"),
        ),
        out_specs=(P(None, "tp", "fsdp"), P(None, "tp", "fsdp")),
        check_vma=False,
    )
```
